64 devices in a mesh: dp: 4 (over x, y), tp: 16 (over z, core).
Axes of the slice: x: 2, y: 2, z: 8, core: 2. Of those that a mesh axis runs over, the one named last changes fastest.
The devices are a block of a 4x4x8 slice.
Arguments:
- hidden: bfloat16 [32768, 2048], P(('dp', 'tp')), parts along dimension 0
- norm_scale: float32 [2048], replicated
- embed: bfloat16 [151936, 2048], P('tp')
- target: int32 [32768], P(('dp', 'tp')), parts along dimension 0
Outputs:
- output 1: float32 [32768], P(('dp', 'tp')), parts along dimension 0
- output 2: float32 [32768], P(('dp', 'tp')), parts along dimension 0
There are 4 independent parts. The reference program is written for one: setup_inputs(seed, part) draws one part's arguments, and reference() takes and returns one part's arrays. A program takes and returns all parts, laid end to end along the dimension named above; an argument that names none is the same for every part.
All inputs are finite; a program needn't handle non-finite values.
Results may differ from the reference program's by a relative error of at most 0.001.
Values are sent between devices in bfloat16 or wider.
A program may use at most 768 MiB of HBM per device.

```python
import math
import jax
import jax.numpy as jnp
from jax import lax

TOK_DEV = 512
GROUP_SIZE = 16
VOCAB_SIZE = 151936
MODEL_DIM = 2048

N_TOK = TOK_DEV * GROUP_SIZE
ROW_BLOCK = min(TOK_DEV, 64)
ROW_GROUPS = 16
NORM_EPS = 1e-5
OUT_SCALE = 0.5773502691896257
ROW_NORM = 2.0


def draw_targets(key):
    words = jax.random.randint(key, (N_TOK,), 0, VOCAB_SIZE, jnp.int32)
    return words.at[0].set(0).at[N_TOK - 1].set(VOCAB_SIZE - 1)


def draw_table(key):
    group_keys = jax.random.split(key, ROW_GROUPS)

    def one_group(group_key):
        values = jax.random.normal(group_key, (VOCAB_SIZE // ROW_GROUPS, MODEL_DIM), jnp.float32)
        return (values * (ROW_NORM / math.sqrt(MODEL_DIM))).astype(jnp.bfloat16)

    return lax.map(one_group, group_keys).reshape(VOCAB_SIZE, MODEL_DIM)


def setup_inputs(seed: int = 0, part: int = 0) -> dict:
    base_key = jax.random.key(seed)
    part_key = jax.random.fold_in(base_key, part)
    emb_key, scale_key = jax.random.split(base_key, 2)
    noise_key, tgt_key, boost_key = jax.random.split(part_key, 3)
    embed = draw_table(emb_key)
    norm_scale = 1.0 + 0.2 * jax.random.normal(scale_key, (MODEL_DIM,), jnp.float32)
    target = draw_targets(tgt_key)
    offset = jax.random.uniform(boost_key, (N_TOK,), jnp.float32, -2.5, 1.5)
    spread = OUT_SCALE * ROW_NORM
    tgt_boost = (math.log(VOCAB_SIZE) + 0.5 * spread * spread + offset) / (OUT_SCALE * ROW_NORM * ROW_NORM)
    noise = jax.random.normal(noise_key, (N_TOK, MODEL_DIM), jnp.float32)
    tgt_rows = embed[target].astype(jnp.float32)
    hidden = (noise + tgt_boost[:, None] * tgt_rows).astype(jnp.bfloat16)
    return {"hidden": hidden, "norm_scale": norm_scale, "embed": embed, "target": target}


def reference(hidden, norm_scale, embed, target):
    rows = hidden.astype(jnp.float32)
    mean_sq = jnp.mean(rows * rows, axis=-1, keepdims=True)
    normed = (rows * lax.rsqrt(mean_sq + NORM_EPS) * norm_scale).astype(jnp.bfloat16)
    row_blocks = normed.reshape(N_TOK // ROW_BLOCK, ROW_BLOCK, MODEL_DIM)
    tgt_blocks = target.reshape(N_TOK // ROW_BLOCK, ROW_BLOCK)

    def one_block(block):
        block_rows, block_tgt = block
        logits = jnp.dot(block_rows, embed.T, preferred_element_type=jnp.float32) * OUT_SCALE
        log_sum = jax.nn.logsumexp(logits, axis=-1)
        tgt_logit = jnp.take_along_axis(logits, block_tgt[:, None], axis=1)[:, 0]
        return tgt_logit - log_sum, log_sum

    log_prob, log_sum = lax.map(one_block, (row_blocks, tgt_blocks))
    return log_prob.reshape(N_TOK), log_sum.reshape(N_TOK)
```

```python
import functools
import math

import jax
import jax.numpy as jnp
from jax import lax
from jax.experimental import pallas as pl
from jax.experimental.pallas import tpu as pltpu
from jax.sharding import PartitionSpec as P

NORM_EPS = 1e-5
OUT_SCALE = 0.5773502691896257
LOG2E = 1.0 / math.log(2.0)
LN2 = math.log(2.0)
PIECE = 72
CHUNK = 288
TRIP = 11 * CHUNK
COLS = 256
MESH = pl.DeviceIdType.MESH


def kernel(n_dev, hidden, gain, embed, target, log_prob, log_sum, blocks,
           tab, act, even, odd, tail, stats, ids, outbox, inbox, words,
           row_sem, save_sem, tab_sem, act_sem, recv_sem, ring_sem, pair_sem, word_out, word_in, box_out, box_in):
    rows, dim = embed.shape
    tok = hidden.shape[0]
    n_trip = pl.cdiv(rows, TRIP)
    pad = n_trip * TRIP - rows
    me = lax.axis_index("tp")
    chip, core = lax.div(me, 2), lax.rem(me, 2)
    n_chip = n_dev // 2
    way = 1 - 2 * core
    ahead = lax.rem(chip + way + n_chip, n_chip) * 2 + core
    pair = chip * 2 + 1 - core

    def owner(j):
        hop = lax.div(j + 2, 4)
        side = 1 - 2 * lax.rem(j, 2)
        at = lax.rem(chip - way * side * hop + n_chip, n_chip)
        late = lax.div(j + n_dev - 2, n_dev)
        return at * 2 + lax.rem(core + lax.div(j, 2) + lax.rem(j, 2) + late, 2)

    def send_block(src, slot, sem, dev):
        return pltpu.make_async_remote_copy(
            src_ref=src, dst_ref=blocks.at[slot], send_sem=sem, recv_sem=recv_sem.at[slot],
            device_id={"tp": dev}, device_id_type=MESH)

    def send_words(dev):
        return pltpu.make_async_remote_copy(
            src_ref=target, dst_ref=words.at[me], send_sem=word_out.at[dev], recv_sem=word_in.at[me],
            device_id={"tp": dev}, device_id_type=MESH)

    def recv_words(dev):
        return pltpu.make_async_remote_copy(
            src_ref=target, dst_ref=words.at[dev], send_sem=word_out.at[dev], recv_sem=word_in.at[dev],
            device_id={"tp": dev}, device_id_type=MESH)

    def send_stats(j, dev):
        return pltpu.make_async_remote_copy(
            src_ref=outbox.at[j], dst_ref=inbox.at[me], send_sem=box_out.at[j], recv_sem=box_in.at[me],
            device_id={"tp": dev}, device_id_type=MESH)

    def recv_stats(dev):
        return pltpu.make_async_remote_copy(
            src_ref=outbox.at[0], dst_ref=inbox.at[dev], send_sem=box_out.at[0], recv_sem=box_in.at[dev],
            device_id={"tp": dev}, device_id_type=MESH)

    def load_table(t, n):
        at = pl.ds(pl.multiple_of(t * TRIP, 8), n)
        return pltpu.make_async_copy(embed.at[at], tab.at[at], tab_sem.at[t])

    def load_act(j):
        return pltpu.make_async_copy(blocks.at[lax.rem(j, n_dev)], act.at[lax.rem(j, 2)], act_sem)

    def place(j):
        other = lax.div(lax.rem(j, n_dev) + n_dev - 1, n_dev)
        return other * lax.rem(j, 2) + 2 * (1 - other)

    def prepare(slot, dev):
        local = words[dev] - me * rows
        local = jnp.where((local >= 0) & (local < rows), local, -TRIP * n_trip)
        local = jnp.broadcast_to(local, (8, tok)) - lax.broadcasted_iota(jnp.int32, (8, tok), 0)
        ids[slot] = local.astype(jnp.float32)
        stats[slot, 0] = jnp.full((8, tok), -jnp.inf, jnp.float32)
        stats[slot, 1] = jnp.zeros((8, tok), jnp.float32)
        stats[slot, 2] = jnp.zeros((8, tok), jnp.float32)

    def finish(slot):
        part_max, part_sum, part_tgt = stats[slot, 0], stats[slot, 1], stats[slot, 2]
        top = jnp.max(part_max, axis=0, keepdims=True)
        total = jnp.sum(part_sum * jnp.exp2(part_max - top), axis=0, keepdims=True)
        tgt = jnp.sum(part_tgt, axis=0, keepdims=True)
        return top, total, tgt

    def fill(ref, at, values):
        for i, v in enumerate(values):
            ref[at, pl.ds(i, 1), :] = v

    def product(ref, at_zero, base, slot):
        at = pl.ds(pl.multiple_of(base, 16), CHUNK)
        ref[at_zero] = lax.dot_general(tab[at, :], act[slot], (((1,), (1,)), ((), ())),
                                       preferred_element_type=jnp.float32)

    def columns(slot):
        return [[stats[slot, i, :, c:c + COLS] for i in range(3)] for c in range(0, tok, COLS)]

    def keep(slot, vals):
        for q, val in enumerate(vals):
            for i in range(3):
                stats[slot, i, :, q * COLS:(q + 1) * COLS] = val[i]

    def epilogue(ref, at_zero, vals, slot, base, final):
        wait = 0.0
        for p in range(0, CHUNK, PIECE):
            for q, (top, total, tgt) in enumerate(vals):
                cols = slice(q * COLS, (q + 1) * COLS)
                word = (ids[slot, :, cols] - lax.convert_element_type(base, jnp.float32)) + wait
                scale = OUT_SCALE * LOG2E + wait
                raw = [ref[at_zero, i:i + 8, cols] for i in range(p, p + PIECE, 8)]
                log2 = [r * scale for r in raw]
                if final and p == CHUNK - PIECE:
                    for i in range(pad // 8):
                        log2[-1 - i] = jnp.where(base + (CHUNK - 8 * i) > rows, -jnp.inf, log2[-1 - i])
                new = jnp.maximum(top, functools.reduce(jnp.maximum, log2))
                terms = [jnp.exp2(v - new) for v in log2]
                total = total * jnp.exp2(top - new) + functools.reduce(jnp.add, terms)
                wait = total * 0.0
                for i, r in enumerate(raw):
                    tgt = jnp.where(word == float(p + 8 * i), r, tgt)
                vals[q] = [new, total, tgt]
        return vals

    def deliver(j):
        fill(outbox, j, finish(lax.rem(j, 2)))
        send_stats(j, owner(j)).start()

    barrier = pltpu.get_barrier_semaphore()
    for i in range(1, n_dev):
        pl.semaphore_signal(barrier, inc=1, device_id={"tp": lax.rem(me + i, n_dev)}, device_id_type=MESH)
    rows_in = pltpu.make_async_copy(hidden, act.at[0], row_sem)
    rows_in.start()
    for t in range(n_trip):
        load_table(t, min(TRIP, rows - t * TRIP)).start()
    words[me] = target[...]
    prepare(2, me)
    for i in range(3):
        stats[1, i] = jnp.zeros((8, tok), jnp.float32)
    ids[1] = jnp.zeros((8, tok), jnp.float32)
    rows_in.wait()

    def norm(i, _):
        at = pl.ds(pl.multiple_of(i * 16, 16), 16)
        x = act[0, at, :].astype(jnp.float32)
        mean_sq = jnp.mean(x * x, axis=-1, keepdims=True)
        act[0, at, :] = (x * lax.rsqrt(mean_sq + NORM_EPS) * gain[...]).astype(jnp.bfloat16)
        return 0

    lax.fori_loop(0, tok // 16, norm, 0, unroll=4)
    own_save = pltpu.make_async_copy(act.at[0], blocks.at[0], save_sem)
    own_pair = send_block(act.at[0], 1, pair_sem.at[0], pair)
    own_ring = send_block(act.at[0], 2, ring_sem.at[0], ahead)
    pl.semaphore_wait(barrier, n_dev - 1)
    own_pair.start()
    own_ring.start()
    own_save.start()
    for i in range(1, n_dev):
        send_words(lax.rem(me + i, n_dev)).start()
    tail[...] = jnp.zeros_like(tail)

    last = n_dev - 1
    n_step = n_dev * n_trip

    def fetch(k):
        send_block(blocks.at[0], k, pair_sem.at[0], pair).wait_recv()
        load_act(k).start()

    def step(g, _):
        h = g + lax.div(g + n_step - n_trip + 1, n_step)
        j, t = lax.div(h, n_trip), lax.rem(h, n_trip)
        slot, box = lax.rem(j, 2), place(j)

        for i in range(n_trip):
            @pl.when(g == (i if i < n_trip - 1 else 2 * n_trip - 2))
            def _(i=i):
                load_table(i, min(TRIP, rows - i * TRIP)).wait()

        get = lax.div(g, n_step)

        @pl.when((t == 0) & (j > 0))
        def _():
            load_act(j).wait()

            @pl.when(j < n_dev)
            def _():
                dev = owner(j)
                recv_words(dev).wait_recv()
                prepare(slot, dev)

        @pl.when(j == n_dev)
        def _():
            at = last % 2
            keep(at, epilogue(tail, get, columns(at), at, n_trip * TRIP - CHUNK, True))
            deliver(last)

        @pl.when(g == n_trip - 2)
        def _():
            fetch(1)
            send_block(blocks.at[1], 4, ring_sem.at[1], ahead).start()

        @pl.when(t == n_trip - 1)
        def _():
            @pl.when(j == 1)
            def _():
                own_pair.wait_send()
                own_ring.wait_send()
                own_save.wait()

            @pl.when(j > 1)
            def _():
                deliver(j - 1)

            @pl.when(j == last)
            def _():
                load_act(n_dev).start()

            @pl.when(j < last)
            def _():
                k = j + 1
                fetch(k)

                @pl.when(lax.rem(k, 2) == 0)
                def _():
                    send_block(blocks.at[k], k + 1, pair_sem.at[lax.div(k, 2)], pair).start()

                    @pl.when(k + 4 < n_dev)
                    def _():
                        send_block(blocks.at[k], k + 4, ring_sem.at[lax.div(k, 2) + 1], ahead).start()

        first = lax.div(n_trip - t, n_trip)
        after_own = lax.div(j + n_dev - 1, n_dev) - lax.div(j + n_dev - 2, n_dev)
        base = (t + lax.div(j, n_dev) * (n_trip - 1)) * TRIP
        before = first * (2 * after_own + (1 - after_own) * lax.rem(j + 1, 2)) + (1 - first) * box
        folded = first * (n_trip - after_own) * TRIP + (1 - first) * base - CHUNK
        put = lax.div(t, n_trip)
        product(even, put, base, slot)
        keep(before, epilogue(tail, get, columns(before), before, folded, True))
        vals = columns(box)
        refs = [even, odd] * (TRIP // CHUNK)
        refs[TRIP // CHUNK - 1] = tail
        for i in range(1, TRIP // CHUNK):
            product(refs[i], put, base + i * CHUNK, slot)
            vals = epilogue(refs[i - 1], get, vals, box, base + (i - 1) * CHUNK, False)
        keep(box, vals)
        return 0

    lax.fori_loop(0, n_step, step, 0)
    keep(2, epilogue(tail, 0, columns(2), 2, n_trip * TRIP - CHUNK, True))
    fill(inbox, me, finish(2))

    for i in range(1, n_dev):
        recv_stats(lax.rem(me + i, n_dev)).wait_recv()
    parts = [inbox[i] for i in range(n_dev)]
    top = functools.reduce(jnp.maximum, [p[0:1] for p in parts])
    total = functools.reduce(jnp.add, [p[1:2] * jnp.exp2(p[0:1] - top) for p in parts])
    tgt = functools.reduce(jnp.add, [p[2:3] for p in parts]) * OUT_SCALE
    norm_log = top * LN2 + jnp.log(total)
    log_sum[...] = norm_log
    log_prob[...] = tgt - norm_log
    for i in range(1, n_dev):
        send_words(lax.rem(me + i, n_dev)).wait_send()
        send_stats(i, pair).wait_send()
    for i in range(1, n_dev // 2):
        send_block(blocks.at[0], 0, pair_sem.at[i], pair).wait_send()
        if i < n_dev // 2 - 1:
            send_block(blocks.at[0], 0, ring_sem.at[i], ahead).wait_send()


def solution(mesh):
    n_dev = mesh.shape["tp"]
    row_spec = P(("dp", "tp"))

    def local_part(hidden, norm_scale, embed, target):
        tok, dim = hidden.shape
        rows = embed.shape[0]
        n_trip = pl.cdiv(rows, TRIP)
        dma = pltpu.SemaphoreType.DMA
        vmem = pl.BlockSpec(memory_space=pltpu.VMEM)
        anywhere = pl.BlockSpec(memory_space=pl.ANY)
        one = jax.ShapeDtypeStruct((1, tok), jnp.float32)
        log_prob, log_sum, _ = pl.pallas_call(
            functools.partial(kernel, n_dev),
            out_shape=(one, one, jax.ShapeDtypeStruct((n_dev, tok, dim), jnp.bfloat16)),
            in_specs=[anywhere, vmem, anywhere, vmem],
            out_specs=(vmem, vmem, anywhere),
            scratch_shapes=[
                pltpu.VMEM((n_trip * TRIP, dim), jnp.bfloat16),
                pltpu.VMEM((2, tok, dim), jnp.bfloat16),
                pltpu.VMEM((1, CHUNK, tok), jnp.float32),
                pltpu.VMEM((1, CHUNK, tok), jnp.float32),
                pltpu.VMEM((1, CHUNK, tok), jnp.float32),
                pltpu.VMEM((3, 3, 8, tok), jnp.float32),
                pltpu.VMEM((3, 8, tok), jnp.float32),
                pltpu.VMEM((n_dev, 8, tok), jnp.float32),
                pltpu.VMEM((n_dev, 8, tok), jnp.float32),
                pltpu.VMEM((n_dev, 1, tok), jnp.int32),
                dma, dma, dma((n_trip,)), dma, dma((n_dev,)), dma((n_dev // 2,)), dma((n_dev // 2,)),
                dma((n_dev,)), dma((n_dev,)), dma((n_dev,)), dma((n_dev,)),
            ],
            compiler_params=pltpu.CompilerParams(
                collective_id=0, has_side_effects=True, vmem_limit_bytes=60 * 1024 * 1024),
            name="head",
        )(hidden, norm_scale.reshape(1, dim), embed, target.reshape(1, tok))
        return log_prob.reshape(tok), log_sum.reshape(tok)

    return jax.shard_map(local_part, mesh=mesh,
                         in_specs=(P(("dp", "tp"), None), P(None), P("tp", None), row_spec),
                         out_specs=(row_spec, row_spec), check_vma=False)
```
